256 devices in a mesh: seq: 32 (over z, y), batch: 8 (over x, core).
Axes of the slice: x: 4, y: 4, z: 8, core: 2. Of those that a mesh axis runs over, the one named last changes fastest.
Arguments:
- inputs: bfloat16 [65536, 4096], P(('batch', 'seq')), parts along dimension 0, may hold values from -6 to 6
- recur_weight: bfloat16 [16, 256, 256], replicated, may hold values from -0.375 to 0.375
- input_weight: bfloat16 [16, 256, 256], replicated, may hold values from -0.375 to 0.375
- recur_bias: float32 [4096], replicated, may hold values from -4 to 4
- input_bias: float32 [4096], replicated, may hold values from -4 to 4
- decay_rate: float32 [4096], replicated, may hold values from 1.2207031e-06 to 0.02
- kv_weight: bfloat16 [4096, 512], replicated, may hold values from -61 to 61
Outputs:
- attended: bfloat16 [65536, 4096], P(('batch', 'seq')), parts along dimension 0
The draws below stay inside these ranges and needn't reach their ends.
There are 8 independent parts, one for each index of `batch`. The reference program is written for one: setup_inputs(seed, part) draws one part's arguments, and reference() takes and returns one part's arrays. A program takes and returns all parts, laid end to end along the dimension named above; an argument that names none is the same for every part. Nothing has to cross between parts.
All inputs are finite; a program needn't handle non-finite values.
Results may differ from the reference program's by a relative error of at most 0.03.
Values may be sent and summed in bfloat16 or wider, within the bound.
No kernel may reach another device: no remote copies, remote signals or barrier semaphores. Data moves between devices by JAX's collectives and lax.ppermute only.
A program may use at most 128 MiB of HBM per device.

```python
import math
import jax
import jax.numpy as jnp
from jax import lax

D = 4096
HEAD_DIM = 256
BLOCKS = 16
BLOCK_WIDTH = 256
WINDOW = 2048
TOK_DEV = 256
SEQ_LEN = 8192


def draw_kv_weight(key, part):
    first, second = jax.random.split(jax.random.fold_in(key, 7331))
    heads = D // HEAD_DIM
    base = jax.random.normal(first, (D, 2 * HEAD_DIM), jnp.float32) * D ** (-0.5)
    base = jnp.clip(base, -6.0 * D ** (-0.5), 6.0 * D ** (-0.5))
    level = jax.random.uniform(second, (heads,), jnp.float32)
    lowest = 2.0 / HEAD_DIM ** 0.5
    highest = 24.0 / HEAD_DIM ** 0.5
    strength = jnp.exp(jnp.log(lowest) + level * (jnp.log(highest) - jnp.log(lowest)))
    identity = jnp.eye(HEAD_DIM, dtype=jnp.float32)
    aligned = (strength[:, None, None] * identity[None, :, :]).reshape(D, HEAD_DIM)
    key_cols = base[:, :HEAD_DIM] + aligned
    return jnp.concatenate([key_cols, base[:, HEAD_DIM:]], axis=1).astype(jnp.bfloat16)


def shard_levels(rng, shape, cuts, low, top_value):
    def one(dim, blocks):
        steps = jax.random.uniform(jax.random.fold_in(jax.random.fold_in(rng, 6), dim), (blocks,), jnp.float32, low / len(cuts), top_value / len(cuts))
        return jnp.repeat(jnp.exp(steps), shape[dim] // blocks).reshape((-1,) + (1,) * (len(shape) - dim - 1))

    loudness = one(*cuts[0])
    for cut in cuts[1:]:
        loudness = loudness * one(*cut)
    return loudness


def noise(own_key, dims, deviation, limit, shards=(), kind=jnp.bfloat16):
    level = shard_levels(own_key, dims, shards, -0.22, 0.18) if shards else 1.0
    values = jax.random.normal(own_key, dims, jnp.float32) * deviation * level
    return jnp.minimum(jnp.maximum(values, -limit), limit).astype(kind)


def setup_inputs(seed: int = 0, part: int = 0) -> dict:
    streams_of = jax.random.split(jax.random.key(seed), 8)
    part_splits = jax.random.split(jax.random.fold_in(streams_of[7], part), 8)
    return {
        "inputs": noise(part_splits[0], (SEQ_LEN, D), 1.0, 6.0, ((0, 32),)),
        "recur_weight": noise(streams_of[1], (BLOCKS, BLOCK_WIDTH, BLOCK_WIDTH), BLOCK_WIDTH ** -0.5, 0.375),
        "input_weight": noise(streams_of[2], (BLOCKS, BLOCK_WIDTH, BLOCK_WIDTH), BLOCK_WIDTH ** -0.5, 0.375),
        "recur_bias": noise(streams_of[3], (D,), 1.0, 4.0, (), jnp.float32),
        "input_bias": noise(streams_of[4], (D,), 1.0, 4.0, (), jnp.float32),
        "decay_rate": jnp.clip(jnp.exp(jax.random.uniform(streams_of[5], (D,), jnp.float32, math.log(1.220703097715159e-06), math.log(0.02))), 1.220703097715159e-06, 0.02),
        "kv_weight": draw_kv_weight(jax.random.fold_in(streams_of[7], 71), part),
    }


def combine_steps(earlier, later):
    return (earlier[0] * later[0], later[0] * earlier[1] + later[1])

def block_gate(inputs, weight, bias):
    total_rows = inputs.shape[0]
    split = inputs.astype(jnp.float32).reshape(total_rows, weight.shape[0], weight.shape[1])
    mixed = jnp.einsum('tbi,bio->tbo', split, weight.astype(jnp.float32))
    return jax.nn.sigmoid(mixed.reshape(total_rows, -1) + bias)

def reference(inputs, recur_weight, input_weight, recur_bias, input_bias, decay_rate, kv_weight):
    total_rows = inputs.shape[0]
    width_all = inputs.shape[1]
    recurrence = block_gate(inputs, recur_weight, recur_bias)
    input_gate = block_gate(inputs, input_weight, input_bias)
    decay_step = jnp.exp(-8.0 * recurrence * decay_rate)
    driven = jnp.sqrt(1.0 - decay_step * decay_step) * (input_gate * inputs.astype(jnp.float32))
    cumulative, state = lax.associative_scan(combine_steps, (decay_step, driven), axis=0)
    hidden = state.astype(jnp.bfloat16)
    keyval = jnp.dot(hidden, kv_weight, preferred_element_type=jnp.float32).astype(jnp.bfloat16)
    head_dim = kv_weight.shape[1] // 2
    heads = width_all // head_dim
    reach = (WINDOW + TOK_DEV - 2) // TOK_DEV
    padded = jnp.concatenate([jnp.zeros((reach * TOK_DEV, 2 * head_dim), jnp.bfloat16), keyval], axis=0)
    scale = head_dim ** (-0.5)

    def block_out(index):
        start = (index * TOK_DEV).astype(jnp.int32)
        local_kv = lax.dynamic_slice_in_dim(padded, start, (reach + 1) * TOK_DEV, 0).astype(jnp.float32)
        queries = lax.dynamic_slice_in_dim(hidden, start, TOK_DEV, 0).astype(jnp.float32)
        queries = queries.reshape(TOK_DEV, heads, head_dim).transpose(1, 0, 2)
        keys = local_kv[:, :head_dim]
        values = local_kv[:, head_dim:]
        query_pos = start + jnp.arange(TOK_DEV, dtype=jnp.int32)
        key_pos = start - reach * TOK_DEV + jnp.arange((reach + 1) * TOK_DEV, dtype=jnp.int32)
        allowed = (key_pos[None, :] <= query_pos[:, None]) & (key_pos[None, :] > query_pos[:, None] - WINDOW) & (key_pos[None, :] >= 0)
        scores = jnp.einsum('htd,kd->htk', queries, keys) * scale
        scores = jnp.where(allowed[None], scores, -1e+30)
        highest = lax.optimization_barrier(jnp.max(scores, axis=-1, keepdims=True))
        expo = jnp.exp(scores - highest)
        weights = (expo / lax.optimization_barrier(jnp.sum(expo, axis=-1, keepdims=True))).astype(jnp.bfloat16)
        result = jnp.einsum('htk,kd->htd', weights.astype(jnp.float32), values).astype(jnp.bfloat16)
        return result.transpose(1, 0, 2).reshape(TOK_DEV, width_all)
    blocks_out = lax.map(block_out, jnp.arange(total_rows // TOK_DEV, dtype=jnp.int32))
    return blocks_out.reshape(total_rows, width_all)
```

```python
import functools, math
import jax, jax.numpy as jnp
from jax import lax
from jax.experimental import pallas as pl
from jax.experimental.pallas import tpu as pltpu

F32 = jnp.float32
BF16 = jnp.bfloat16
TOK = 256
LOG2E = 1.4426950408889634


def _perm_matrix(transposed):
    row = lax.broadcasted_iota(jnp.int32, (TOK, TOK), 1 if transposed else 0)
    col = lax.broadcasted_iota(jnp.int32, (TOK, TOK), 0 if transposed else 1)
    return (col == (row % 8) * 32 + row // 8).astype(F32).astype(BF16)


def _gates_kernel(x_ref, rw_ref, iw_ref, rb_ref, ib_ref, rate_ref,
                  state_ref, prod_ref, aex_ref, bex_ref, tot_ref, perm_ref, a_ref, d_ref):
    b = pl.program_id(0)

    @pl.when(b == 0)
    def _():
        perm_ref[...] = _perm_matrix(False)

    width = x_ref.shape[1]
    x = jnp.dot(perm_ref[...], x_ref[...], preferred_element_type=F32)
    xb = x.astype(BF16)
    r = jnp.dot(xb, rw_ref[0], preferred_element_type=F32) + rb_ref[...]
    g = jnp.dot(xb, iw_ref[0], preferred_element_type=F32) + ib_ref[...]
    r = 1.0 / (1.0 + jnp.exp(-r))
    g = 1.0 / (1.0 + jnp.exp(-g))
    a = jnp.exp((-8.0 * r) * rate_ref[...])
    d = jnp.sqrt(1.0 - a * a) * (g * x)
    a_ref[...] = a
    d_ref[...] = d
    p = a_ref[0:8, :]
    s = d_ref[0:8, :]
    prod_ref[0:8, :] = p
    state_ref[0:8, :] = s
    for j in range(1, TOK // 8):
        aj = a_ref[8 * j:8 * j + 8, :]
        p = p * aj
        s = s * aj + d_ref[8 * j:8 * j + 8, :]
        prod_ref[8 * j:8 * j + 8, :] = p
        state_ref[8 * j:8 * j + 8, :] = s
    sub = lax.broadcasted_iota(jnp.int32, (8, width), 0)
    for sh in (1, 2, 4):
        pr = pltpu.roll(p, sh, 0)
        sr = pltpu.roll(s, sh, 0)
        s = jnp.where(sub >= sh, p * sr + s, s)
        p = jnp.where(sub >= sh, p * pr, p)
    aex_ref[...] = jnp.where(sub == 0, 1.0, pltpu.roll(p, 1, 0))
    bex_ref[...] = jnp.where(sub == 0, 0.0, pltpu.roll(s, 1, 0))
    tot_ref[0:1, :] = p[7:8, :]
    tot_ref[1:2, :] = s[7:8, :]


def gates(x, rw, iw, rb, ib, rate):
    tok, width = x.shape
    nb, bw = rw.shape[0], rw.shape[1]
    col = lambda rows: pl.BlockSpec((rows, bw), lambda b: (0, b))
    w = pl.BlockSpec((1, bw, bw), lambda b: (b, 0, 0))
    return pl.pallas_call(
        _gates_kernel,
        grid=(nb,),
        in_specs=[col(tok), w, w, col(1), col(1), col(1)],
        out_specs=[col(tok), col(tok), col(8), col(8), col(2)],
        out_shape=[
            jax.ShapeDtypeStruct((tok, width), F32),
            jax.ShapeDtypeStruct((tok, width), F32),
            jax.ShapeDtypeStruct((8, width), F32),
            jax.ShapeDtypeStruct((8, width), F32),
            jax.ShapeDtypeStruct((2, width), F32),
        ],
        scratch_shapes=[pltpu.VMEM((tok, tok), BF16), pltpu.VMEM((tok, bw), F32), pltpu.VMEM((tok, bw), F32)],
        compiler_params=pltpu.CompilerParams(dimension_semantics=("arbitrary",), vmem_limit_bytes=16 * 2**20),
        cost_estimate=pl.CostEstimate(flops=2 * 3 * tok * width * bw, bytes_accessed=2 * tok * width * 5, transcendentals=5 * tok * width),
        name="gates",
    )(x, rw, iw, rb.reshape(1, -1), ib.reshape(1, -1), rate.reshape(1, -1))


def _kv_kernel(state_ref, prod_ref, aex_ref, bex_ref, carry_ref, w_ref, hid_ref, kv_ref, acc_ref, h_ref):
    b = pl.program_id(0)
    cc = bex_ref[...] + aex_ref[...] * carry_ref[...]
    for j in range(TOK // 8):
        h_ref[8 * j:8 * j + 8, :] = state_ref[8 * j:8 * j + 8, :] + prod_ref[8 * j:8 * j + 8, :] * cc
    hb = h_ref[...].astype(BF16)
    hid_ref[...] = hb
    part = jnp.dot(hb, w_ref[...], preferred_element_type=F32)

    @pl.when(b == 0)
    def _():
        acc_ref[...] = part

    @pl.when(b > 0)
    def _():
        acc_ref[...] += part

    @pl.when(b == pl.num_programs(0) - 1)
    def _():
        hd = w_ref.shape[1] // 2
        k = acc_ref[:, :hd] * (LOG2E * hd ** -0.5)
        kv_ref[:hd, :] = k.T.astype(BF16)
        kv_ref[hd:, :] = acc_ref[:, hd:].astype(BF16)


def kv_project(state, prod, aex, bex, carry, w, bw=512):
    tok, width = state.shape
    n = w.shape[1]
    col = lambda rows: pl.BlockSpec((rows, bw), lambda b: (0, b))
    return pl.pallas_call(
        _kv_kernel,
        grid=(width // bw,),
        in_specs=[col(tok), col(tok), col(8), col(8), col(1), pl.BlockSpec((bw, n), lambda b: (b, 0))],
        out_specs=[col(tok), pl.BlockSpec((n, tok), lambda b: (0, 0))],
        out_shape=[jax.ShapeDtypeStruct((tok, width), BF16), jax.ShapeDtypeStruct((n, tok), BF16)],
        scratch_shapes=[pltpu.VMEM((tok, n), F32), pltpu.VMEM((tok, bw), F32)],
        compiler_params=pltpu.CompilerParams(dimension_semantics=("arbitrary",), vmem_limit_bytes=16 * 2**20),
        cost_estimate=pl.CostEstimate(flops=2 * tok * width * n, bytes_accessed=10 * tok * width, transcendentals=0),
        name="kv_project",
    )(state, prod, aex, bex, carry, w)


def _token(axis):
    r = lax.broadcasted_iota(jnp.int32, (TOK, TOK), axis)
    return (r % 8) * 32 + r // 8


def _attn_kernel(bias_ref, q_ref, *refs):
    kv, (o_ref, s_ref, perm_ref, tri_ref) = refs[:9], refs[9:]
    g = pl.program_id(0)
    n = pl.num_programs(0)
    hd = q_ref.shape[1]

    @pl.when(g == 0)
    def _():
        perm_ref[...] = _perm_matrix(True)
        tri_ref[...] = (_token(1) <= _token(0)).astype(F32)
        s_ref[...] = jnp.zeros_like(s_ref)

    slot = lax.rem(g, 2)
    prev = 1 - slot
    q = q_ref[...]
    tri = tri_ref[...] > 0.5
    own = jnp.dot(q, kv[0][:hd, :], preferred_element_type=F32)
    old = jnp.dot(q, kv[8][:hd, :], preferred_element_type=F32) + bias_ref[8]
    s_ref[slot, 0] = jnp.where(tri, own, old)
    for d in range(1, 8):
        s_ref[slot, d] = jnp.dot(q, kv[d][:hd, :], preferred_element_type=F32) + bias_ref[d]
    m = s_ref[prev, 0]
    for d in range(1, 8):
        m = jnp.maximum(m, s_ref[prev, d])
    m = jnp.max(m, axis=1, keepdims=True)
    p = jnp.exp2(s_ref[prev, 0] - m)
    l = p
    pt = jnp.where(tri, p, 0.0).astype(BF16)
    po = jnp.where(tri, 0.0, p).astype(BF16)
    acc = jnp.dot(pt, kv[0][hd:, :], preferred_element_type=F32)
    acc += jnp.dot(po, kv[8][hd:, :], preferred_element_type=F32)
    for d in range(1, 8):
        p = jnp.exp2(s_ref[prev, d] - m)
        l = l + p
        acc += jnp.dot(p.astype(BF16), kv[d][hd:, :], preferred_element_type=F32)
    l = jnp.sum(l, axis=1, keepdims=True)
    o = (acc * (1.0 / l)).astype(BF16)
    o_ref[...] = jnp.dot(perm_ref[...], o, preferred_element_type=F32).astype(BF16)


def attention(hidden, kv, bias):
    tok, width = hidden.shape
    hd = kv[0].shape[0] // 2
    heads = width // hd
    nb = len(kv)
    return pl.pallas_call(
        _attn_kernel,
        grid_spec=pltpu.PrefetchScalarGridSpec(
            num_scalar_prefetch=1,
            grid=(heads + 1,),
            in_specs=[
                pl.BlockSpec((tok, hd), lambda g, *_: (0, jnp.minimum(g, heads - 1))),
                *[pl.BlockSpec((2 * hd, tok), lambda g, *_: (0, 0)) for _ in kv],
            ],
            out_specs=pl.BlockSpec((tok, hd), lambda g, *_: (0, jnp.maximum(g - 1, 0))),
            scratch_shapes=[
                pltpu.VMEM((2, 8, tok, tok), F32),
                pltpu.VMEM((tok, tok), BF16),
                pltpu.VMEM((tok, tok), F32),
            ],
        ),
        out_shape=jax.ShapeDtypeStruct((tok, width), BF16),
        compiler_params=pltpu.CompilerParams(dimension_semantics=("arbitrary",), vmem_limit_bytes=32 * 2**20),
        cost_estimate=pl.CostEstimate(flops=4 * tok * width * nb * tok, bytes_accessed=4 * tok * width, transcendentals=8 * tok * tok * heads),
        name="attention",
    )(bias, hidden, *kv)


def _after(earlier, later):
    return (earlier[0] * later[0], later[0] * earlier[1] + later[1])


def _kept(keep, pair):
    return (jnp.where(keep, pair[0], 1.0), jnp.where(keep, pair[1], 0.0))


def _shift(value, axis, distance):
    size = lax.axis_size(axis)
    return lax.ppermute(value, axis, [(i, (i + distance) % size) for i in range(size)])


def _entering(total):
    pair = lambda v: (v[0:1], v[1:2])
    y, z = lax.axis_index("y"), lax.axis_index("z")
    ny, nz = lax.axis_size("y"), lax.axis_size("z")
    near = {k: pair(_shift(total, "y", k)) for k in range(ny - 1, 0, -1)}
    row = (jnp.ones_like(total[0:1]), jnp.zeros_like(total[0:1]))
    for k in range(ny - 1, 0, -1):
        row = _after(row, _kept(y >= k, near[k]))
    whole = _after(row, pair(total))
    for k in range(ny - 1, 0, -1):
        whole = _after(whole, _kept(y < k, near[k]))
    before = (jnp.ones_like(total[0:1]), jnp.zeros_like(total[0:1]))
    step = 1
    while step < nz:
        sent = jnp.concatenate(_after(before, whole))
        before = _after(_kept(z >= step, pair(_shift(sent, "z", step))), before)
        step *= 2
    return row[0] * before[1] + row[1]


def _window(kv):
    y = lax.axis_index("y")
    ny = lax.axis_size("y")
    one = _shift(kv, "z", 1)
    two = _shift(one, "z", 1)
    blocks, back = [], []
    for k in (1, 3, 2):
        blocks.append(_shift(one, "y", k))
        back.append(jnp.where(y >= k, ny + k, k))
    blocks.append(one)
    back.append(jnp.full((), ny, jnp.int32))
    for k in (1, 3, 2):
        blocks.append(_shift(jnp.where(y + k < ny, kv, two), "y", k))
        back.append(jnp.where(y >= k, k, ny + k))
    blocks.append(two)
    back.append(jnp.full((), 2 * ny, jnp.int32))
    return blocks, back


def _on_device(inputs, recur_weight, input_weight, recur_bias, input_bias, decay_rate, kv_weight):
    state, prod, aex, bex, total = gates(inputs, recur_weight, input_weight, recur_bias, input_bias, decay_rate)
    carry = _entering(total)
    hidden, kv = kv_project(state, prod, aex, bex, carry, kv_weight)
    blocks, back = _window(kv)
    place = lax.axis_index("z") * lax.axis_size("y") + lax.axis_index("y")
    bias = jnp.where(place >= jnp.stack([jnp.zeros((), jnp.int32), *back]), 0.0, -1e30).astype(F32)
    return attention(hidden, [kv, *blocks], bias)


def solution(mesh):
    ny = 4
    nb, ns = mesh.shape["batch"], mesh.shape["seq"]
    names = mesh.axis_names
    order = {"seq": ("z", "y"), "batch": ("batch",)}
    sizes = {"seq": (ns // ny, ny), "batch": (nb,)}
    fine = jax.sharding.Mesh(
        mesh.devices.reshape([n for a in names for n in sizes[a]]),
        [a for n in names for a in order[n]],
    )
    rows = jax.sharding.PartitionSpec(("batch", "z", "y"), None)
    rep = jax.sharding.PartitionSpec()
    return jax.shard_map(
        _on_device, mesh=fine, in_specs=(rows, rep, rep, rep, rep, rep, rep), out_specs=rows, check_vma=False
    )
```

```python
import functools, math
import jax, jax.numpy as jnp
from jax import lax
from jax.experimental import pallas as pl
from jax.experimental.pallas import tpu as pltpu

F32 = jnp.float32
BF16 = jnp.bfloat16
TOK = 256
LOG2E = 1.4426950408889634


def _perm_matrix(transposed):
    row = lax.broadcasted_iota(jnp.int32, (TOK, TOK), 1 if transposed else 0)
    col = lax.broadcasted_iota(jnp.int32, (TOK, TOK), 0 if transposed else 1)
    return (col == (row % 8) * 32 + row // 8).astype(F32).astype(BF16)


def _gates_kernel(x_ref, rw_ref, iw_ref, rb_ref, ib_ref, rate_ref,
                  state_ref, prod_ref, aex_ref, bex_ref, tot_ref, perm_ref, a_ref, d_ref):
    @pl.when(pl.program_id(0) == 0)
    def _():
        perm_ref[...] = _perm_matrix(False)

    count, bw = rw_ref.shape[0], rw_ref.shape[1]
    for i in range(count):
        at = slice(i * bw, (i + 1) * bw)
        x = jnp.dot(perm_ref[...], x_ref[:, at], preferred_element_type=F32)
        xb = x.astype(BF16)
        r = jnp.dot(xb, rw_ref[i], preferred_element_type=F32)
        g = jnp.dot(xb, iw_ref[i], preferred_element_type=F32)
        r = 1.0 / (1.0 + jnp.exp2(r * -LOG2E + rb_ref[:, at] * -LOG2E))
        g = 1.0 / (1.0 + jnp.exp2(g * -LOG2E + ib_ref[:, at] * -LOG2E))
        a = jnp.exp2(r * (rate_ref[:, at] * (-8.0 * LOG2E)))
        left = 1.0 - a * a
        a_ref[:, at] = a
        d_ref[:, at] = (left * lax.rsqrt(jnp.maximum(left, 1e-30))) * (g * x)
    width = count * bw
    for c in range(0, width, LANES):
        at = slice(c, c + LANES)
        p = a_ref[0:8, at]
        s = d_ref[0:8, at]
        prod_ref[0:8, at] = p
        state_ref[0:8, at] = s
        for j in range(1, TOK // 8):
            row = slice(8 * j, 8 * j + 8)
            aj = a_ref[row, at]
            p = p * aj
            s = s * aj + d_ref[row, at]
            prod_ref[row, at] = p
            state_ref[row, at] = s
        sub = lax.broadcasted_iota(jnp.int32, (8, LANES), 0)
        for sh in (1, 2, 4):
            pr = pltpu.roll(p, sh, 0)
            sr = pltpu.roll(s, sh, 0)
            s = jnp.where(sub >= sh, p * sr + s, s)
            p = jnp.where(sub >= sh, p * pr, p)
        aex_ref[:, at] = jnp.where(sub == 0, 1.0, pltpu.roll(p, 1, 0))
        bex_ref[:, at] = jnp.where(sub == 0, 0.0, pltpu.roll(s, 1, 0))
        tot_ref[0:1, at] = p[7:8, :]
        tot_ref[1:2, at] = s[7:8, :]


LANES = 256
BLOCKS_A_STEP = 4


def gates(x, rw, iw, rb, ib, rate):
    tok, width = x.shape
    nb, bw = rw.shape[0], rw.shape[1]
    count = BLOCKS_A_STEP
    col = lambda rows: pl.BlockSpec((rows, count * bw), lambda b: (0, b))
    w = pl.BlockSpec((count, bw, bw), lambda b: (b, 0, 0))
    return pl.pallas_call(
        _gates_kernel,
        grid=(nb // count,),
        in_specs=[col(tok), w, w, col(1), col(1), col(1)],
        out_specs=[col(tok), col(tok), col(8), col(8), col(2)],
        out_shape=[
            jax.ShapeDtypeStruct((tok, width), F32),
            jax.ShapeDtypeStruct((tok, width), F32),
            jax.ShapeDtypeStruct((8, width), F32),
            jax.ShapeDtypeStruct((8, width), F32),
            jax.ShapeDtypeStruct((2, width), F32),
        ],
        scratch_shapes=[pltpu.VMEM((tok, tok), BF16), pltpu.VMEM((tok, count * bw), F32), pltpu.VMEM((tok, count * bw), F32)],
        compiler_params=pltpu.CompilerParams(dimension_semantics=("arbitrary",), vmem_limit_bytes=60 * 2**20),
        cost_estimate=pl.CostEstimate(flops=2 * 3 * tok * width * bw, bytes_accessed=2 * tok * width * 5, transcendentals=5 * tok * width),
        name="gates",
    )(x, rw, iw, rb.reshape(1, -1), ib.reshape(1, -1), rate.reshape(1, -1))


def _kv_kernel(state_ref, prod_ref, aex_ref, bex_ref, carry_ref, w_ref, hid_ref, kv_ref, acc_ref, h_ref, perm_ref):
    b = pl.program_id(0)

    @pl.when(b == 0)
    def _():
        perm_ref[...] = _perm_matrix(True)

    cc = bex_ref[...] + aex_ref[...] * carry_ref[...]
    for j in range(TOK // 8):
        row = slice(8 * j, 8 * j + 8)
        h_ref[row, :] = state_ref[row, :] + prod_ref[row, :] * cc
    hb = jnp.dot(perm_ref[...], h_ref[...].astype(BF16), preferred_element_type=F32).astype(BF16)
    hid_ref[...] = hb
    part = jnp.dot(hb, w_ref[...], preferred_element_type=F32)

    @pl.when(b == 0)
    def _():
        acc_ref[...] = part

    @pl.when(b > 0)
    def _():
        acc_ref[...] += part

    @pl.when(b == pl.num_programs(0) - 1)
    def _():
        hd = w_ref.shape[1] // 2
        k = acc_ref[:, :hd] * (LOG2E * hd ** -0.5)
        kv_ref[:hd, :] = k.T.astype(BF16)
        kv_ref[hd:, :] = acc_ref[:, hd:].astype(BF16)


def kv_project(state, prod, aex, bex, carry, w, bw=2048):
    tok, width = state.shape
    n = w.shape[1]
    col = lambda rows: pl.BlockSpec((rows, bw), lambda b: (0, b))
    return pl.pallas_call(
        _kv_kernel,
        grid=(width // bw,),
        in_specs=[col(tok), col(tok), col(8), col(8), col(1), pl.BlockSpec((bw, n), lambda b: (b, 0))],
        out_specs=[col(tok), pl.BlockSpec((n, tok), lambda b: (0, 0))],
        out_shape=[jax.ShapeDtypeStruct((tok, width), BF16), jax.ShapeDtypeStruct((n, tok), BF16)],
        scratch_shapes=[pltpu.VMEM((tok, n), F32), pltpu.VMEM((tok, bw), F32), pltpu.VMEM((tok, tok), BF16)],
        compiler_params=pltpu.CompilerParams(dimension_semantics=("arbitrary",), vmem_limit_bytes=60 * 2**20),
        cost_estimate=pl.CostEstimate(flops=2 * tok * width * n, bytes_accessed=10 * tok * width, transcendentals=0),
        name="kv_project",
    )(state, prod, aex, bex, carry, w)


class _Part:
    def __init__(self, count, edges, merge):
        self.count, self.edges, self.merge = count, edges, merge

    def scores(self, q, d, kv, bias_ref, s_ref):
        hd = kv[0].shape[0] // 2
        s = jnp.dot(q, kv[d][:hd, :], preferred_element_type=F32)
        s_ref[:, d * TOK:(d + 1) * TOK] = s if self.edges and d == 0 else s + bias_ref[d]

    def weights(self, r, s_ref, p_ref, r_ref, w_ref, tri_ref, lse_ref):
        cols = self.count * TOK
        at = slice(r, r + ROWS)
        row = slice(r % TOK, r % TOK + ROWS)
        lane = slice(r // TOK * 128, r // TOK * 128 + 128)
        last = cols - TOK
        merged = []
        if self.edges:
            keep = [tri_ref[row, c:c + 128] > 0.5 for c in range(0, TOK, 128)]
            merged = [
                jnp.where(keep[i], s_ref[at, 128 * i:128 * i + 128], s_ref[at, last + 128 * i:last + 128 * i + 128])
                for i in range(2)
            ]
        plain = range(TOK, last, 128) if self.edges else range(0, cols, 128)
        m = lse_ref[row, lane] if self.merge else None
        for v in merged:
            m = v if m is None else jnp.maximum(m, v)
        for c in plain:
            v = s_ref[at, c:c + 128]
            m = v if m is None else jnp.maximum(m, v)
        m = jnp.max(m, axis=1, keepdims=True)
        l = None
        for i, v in enumerate(merged):
            p = jnp.exp2(v - m)
            l = p if l is None else l + p
            p_ref[at, 128 * i:128 * i + 128] = jnp.where(keep[i], p, 0.0).astype(BF16)
            p_ref[at, last + 128 * i:last + 128 * i + 128] = jnp.where(keep[i], 0.0, p).astype(BF16)
        for c in plain:
            p = jnp.exp2(s_ref[at, c:c + 128] - m)
            l = p if l is None else l + p
            p_ref[at, c:c + 128] = p.astype(BF16)
        l = jnp.broadcast_to(jnp.sum(l, axis=1, keepdims=True), (ROWS, 128))
        if self.merge:
            before = jnp.exp2(lse_ref[row, lane] - m)
            l = l + before
            w_ref[at, :] = before / l
        else:
            lse_ref[row, lane] = m + jnp.log2(l)
        r_ref[at, :] = 1.0 / l

    def values(self, d, p_ref, kv):
        hd = kv[0].shape[0] // 2
        return jnp.dot(p_ref[:, d * TOK:(d + 1) * TOK], kv[d][hd:, :], preferred_element_type=F32)

    def kernel(self, bias_ref, q_ref, *refs):
        kv, refs = refs[:self.count], refs[self.count:]
        if self.merge:
            (lse_ref, before_ref, o_ref), refs = refs[:3], refs[3:]
        else:
            (o_ref, lse_ref), refs = refs[:2], refs[2:]
        s0, s1, p0, p1, r0, r1, w0, w1, tri_ref = refs
        s, p, inv, w = (s0, s1), (p0, p1), (r0, r1), (w0, w1)
        t = pl.program_id(0)
        last = pl.num_programs(0) - 3
        even = lax.rem(t, 2) == 0
        hd = kv[0].shape[0] // 2

        @pl.when(t == 0)
        def _():
            row = lax.broadcasted_iota(jnp.int32, (TOK, TOK), 0)
            col = lax.broadcasted_iota(jnp.int32, (TOK, TOK), 1)
            tri_ref[...] = (col <= row).astype(F32)

        def step(a, score, weigh, value):
            b = 1 - a
            total = UNIT * TOK // ROWS
            done, acc = 0, None
            if score:
                q = jnp.concatenate([q_ref[:, i * hd:(i + 1) * hd] for i in range(UNIT)], axis=0)
            for d in range(self.count):
                if score:
                    self.scores(q, d, kv, bias_ref, s[a])
                if value:
                    part = self.values(d, p[a], kv)
                    acc = part if acc is None else acc + part
                while weigh and done * self.count < (d + 1) * total:
                    self.weights(done * ROWS, s[b], p[b], inv[b], w[b], tri_ref, lse_ref)
                    done += 1
            if value:
                wide = lambda v: jnp.concatenate([v] * (hd // 128), axis=1)
                o = acc * wide(inv[a][...])
                for i in range(UNIT):
                    col, row = slice(i * hd, (i + 1) * hd), slice(i * TOK, (i + 1) * TOK)
                    part = o[row, :]
                    if self.merge:
                        part = part + before_ref[:, col] * wide(w[a][row, :])
                    o_ref[:, col] = part.astype(o_ref.dtype)

        pl.when(t == 0)(lambda: step(0, True, False, False))
        pl.when(t == 1)(lambda: step(1, True, True, False))
        pl.when((t >= 2) & (t <= last) & even)(lambda: step(0, True, True, True))
        pl.when((t >= 2) & (t <= last) & ~even)(lambda: step(1, True, True, True))
        pl.when(t == last + 1)(lambda: step(0, False, True, True))
        pl.when(t == last + 2)(lambda: step(1, False, False, True))

    def __call__(self, hidden, kv, bias, earlier=()):
        tok, width = hidden.shape
        hd = kv[0].shape[0] // 2
        heads = width // hd
        units = heads // UNIT
        unit = UNIT * tok
        block = lambda cols, lag: pl.BlockSpec((tok, UNIT * cols), lambda t, *_: (0, jnp.clip(t - lag, 0, units - 1)))
        result = jax.ShapeDtypeStruct((tok, width), BF16)
        out_specs, out_shape = block(hd, 2), result
        if not self.merge:
            out_specs = [block(hd, 2), block(128, 1)]
            out_shape = [jax.ShapeDtypeStruct((tok, width), F32), jax.ShapeDtypeStruct((tok, heads * 128), F32)]
        return pl.pallas_call(
            self.kernel,
            grid_spec=pltpu.PrefetchScalarGridSpec(
                num_scalar_prefetch=1,
                grid=(units + 2,),
                in_specs=[
                    block(hd, 0),
                    *[pl.BlockSpec((2 * hd, tok), lambda t, *_: (0, 0)) for _ in kv],
                    *([block(128, 1), block(hd, 2)] if self.merge else []),
                ],
                out_specs=out_specs,
                scratch_shapes=[
                    pltpu.VMEM((unit, self.count * tok), F32),
                    pltpu.VMEM((unit, self.count * tok), F32),
                    pltpu.VMEM((unit, self.count * tok), BF16),
                    pltpu.VMEM((unit, self.count * tok), BF16),
                    *[pltpu.VMEM((unit, 128), F32)] * 4,
                    pltpu.VMEM((tok, tok), F32),
                ],
            ),
            out_shape=out_shape,
            compiler_params=pltpu.CompilerParams(
                dimension_semantics=("arbitrary",),
                vmem_limit_bytes=ATTN_MIB * 2**20,
            ),
            cost_estimate=pl.CostEstimate(flops=4 * tok * width * self.count * tok, bytes_accessed=8 * tok * width, transcendentals=self.count * tok * tok * heads),
            name="attention_last" if self.merge else "attention_first",
        )(bias, hidden, *kv, *earlier)


ROWS = 32
UNIT = 2
ATTN_MIB = 32
HOIST = 3000


def attention(hidden, kv, bias):
    first, rest = [3, 4, 5, 6], [0, 1, 2, 7, 8]
    values, lse = _Part(4, False, False)(hidden, [kv[i] for i in first], jnp.stack([bias[i] for i in first]))
    return _Part(5, True, True)(hidden, [kv[i] for i in rest], jnp.stack([bias[i] for i in rest]), (lse, values))


def _after(earlier, later):
    return (earlier[0] * later[0], later[0] * earlier[1] + later[1])


def _kept(keep, pair):
    return (jnp.where(keep, pair[0], 1.0), jnp.where(keep, pair[1], 0.0))


def _shift(value, axis, distance):
    size = lax.axis_size(axis)
    return lax.ppermute(value, axis, [(i, (i + distance) % size) for i in range(size)])


def _entering(total):
    pair = lambda v: (v[0:1], v[1:2])
    packed = lambda p: jnp.concatenate(p)
    y, z = lax.axis_index("y"), lax.axis_index("z")
    ny, nz = lax.axis_size("y"), lax.axis_size("z")
    none = (jnp.ones_like(total[0:1]), jnp.zeros_like(total[0:1]))
    near = {k: pair(_shift(total, "y", k)) for k in range(ny - 1, 0, -1)}
    row = none
    for k in range(ny - 1, 0, -1):
        row = _after(row, _kept(y >= k, near[k]))
    whole = _after(row, pair(total))
    for k in range(ny - 1, 0, -1):
        whole = _after(whole, _kept(y < k, near[k]))
    if nz == 8:
        below = pair(_shift(packed(whole), "z", 1))
        above = pair(_shift(packed(whole), "z", -1))
        lower, upper = (z - 1) % nz, (z + 1) % nz

        def sent(target, rows):
            found = none
            for place, value in rows:
                found = _after(found, _kept(place < target, value))
            return packed(found)

        up = sent((z + 3) % nz, [(lower, below), (z, whole), (upper, above)])
        down = sent((z - 3) % nz, [(lower, below), (z, whole)])
        from_below = pair(_shift(up, "z", 3))
        from_above = pair(_shift(down, "z", -3))
        before = _kept(upper < z, above)
        for value in (from_above, from_below, _kept(lower < z, below)):
            before = _after(before, value)
    else:
        before, step = none, 1
        while step < nz:
            sent = packed(_after(before, whole))
            before = _after(_kept(z >= step, pair(_shift(sent, "z", step))), before)
            step *= 2
    return row[0] * before[1] + row[1]


def _window(kv):
    y = lax.axis_index("y")
    ny = lax.axis_size("y")
    one = _shift(kv, "z", 1)
    early = [(_shift(one, "y", k), jnp.where(y >= k, ny + k, k)) for k in (1, 3, 2)]
    two = _shift(one, "z", 1)
    late = [(_shift(jnp.where(y + k < ny, kv, two), "y", k), jnp.where(y >= k, k, ny + k)) for k in (1, 3, 2)]
    found = [*late[:2], (one, jnp.full((), ny, jnp.int32)), *early, late[2], (two, jnp.full((), 2 * ny, jnp.int32))]
    return [b for b, _ in found], [k for _, k in found]


def _on_device(inputs, recur_weight, input_weight, recur_bias, input_bias, decay_rate, kv_weight):
    state, prod, aex, bex, total = gates(inputs, recur_weight, input_weight, recur_bias, input_bias, decay_rate)
    carry = _entering(total)
    hidden, kv = kv_project(state, prod, aex, bex, carry, kv_weight)
    blocks, back = _window(kv)
    place = lax.axis_index("z") * lax.axis_size("y") + lax.axis_index("y")
    bias = [jnp.where(place >= k, 0.0, -1e30).astype(F32) for k in (jnp.zeros((), jnp.int32), *back)]
    return attention(hidden, [kv, *blocks], bias)


def solution(mesh):
    ny = 4
    nb, ns = mesh.shape["batch"], mesh.shape["seq"]
    names = mesh.axis_names
    order = {"seq": ("z", "y"), "batch": ("batch",)}
    sizes = {"seq": (ns // ny, ny), "batch": (nb,)}
    fine = jax.sharding.Mesh(
        mesh.devices.reshape([n for a in names for n in sizes[a]]),
        [a for n in names for a in order[n]],
    )
    rows = jax.sharding.PartitionSpec(("batch", "z", "y"), None)
    rep = jax.sharding.PartitionSpec()
    return jax.shard_map(
        _on_device, mesh=fine, in_specs=(rows, rep, rep, rep, rep, rep, rep), out_specs=rows, check_vma=False
    )
```

```python
import functools, math
import jax, jax.numpy as jnp
from jax import lax
from jax.experimental import pallas as pl
from jax.experimental.pallas import tpu as pltpu

F32 = jnp.float32
BF16 = jnp.bfloat16
TOK = 256
LOG2E = 1.4426950408889634


def _perm_matrix(transposed):
    row = lax.broadcasted_iota(jnp.int32, (TOK, TOK), 1 if transposed else 0)
    col = lax.broadcasted_iota(jnp.int32, (TOK, TOK), 0 if transposed else 1)
    return (col == (row % 8) * 32 + row // 8).astype(F32).astype(BF16)


def _gates_kernel(x_ref, rw_ref, iw_ref, rb_ref, ib_ref, rate_ref,
                  state_ref, prod_ref, aex_ref, bex_ref, tot_ref, perm_ref, a_ref, d_ref):
    @pl.when(pl.program_id(0) == 0)
    def _():
        perm_ref[...] = _perm_matrix(False)

    count, bw = rw_ref.shape[0], rw_ref.shape[1]
    for i in range(count):
        at = slice(i * bw, (i + 1) * bw)
        x = jnp.dot(perm_ref[...], x_ref[:, at], preferred_element_type=F32)
        xb = x.astype(BF16)
        r = jnp.dot(xb, rw_ref[i], preferred_element_type=F32)
        g = jnp.dot(xb, iw_ref[i], preferred_element_type=F32)
        r = 1.0 / (1.0 + jnp.exp2(r * -LOG2E + rb_ref[:, at] * -LOG2E))
        g = 1.0 / (1.0 + jnp.exp2(g * -LOG2E + ib_ref[:, at] * -LOG2E))
        a = jnp.exp2(r * (rate_ref[:, at] * (-8.0 * LOG2E)))
        left = 1.0 - a * a
        a_ref[:, at] = a
        d_ref[:, at] = (left * lax.rsqrt(jnp.maximum(left, 1e-30))) * (g * x)
    width = count * bw
    for c in range(0, width, LANES):
        at = slice(c, c + LANES)
        p = a_ref[0:8, at]
        s = d_ref[0:8, at]
        prod_ref[0:8, at] = p
        state_ref[0:8, at] = s
        for j in range(1, TOK // 8):
            row = slice(8 * j, 8 * j + 8)
            aj = a_ref[row, at]
            p = p * aj
            s = s * aj + d_ref[row, at]
            prod_ref[row, at] = p
            state_ref[row, at] = s
        sub = lax.broadcasted_iota(jnp.int32, (8, LANES), 0)
        for sh in (1, 2, 4):
            pr = pltpu.roll(p, sh, 0)
            sr = pltpu.roll(s, sh, 0)
            s = jnp.where(sub >= sh, p * sr + s, s)
            p = jnp.where(sub >= sh, p * pr, p)
        aex_ref[:, at] = jnp.where(sub == 0, 1.0, pltpu.roll(p, 1, 0))
        bex_ref[:, at] = jnp.where(sub == 0, 0.0, pltpu.roll(s, 1, 0))
        tot_ref[0:1, at] = p[7:8, :]
        tot_ref[1:2, at] = s[7:8, :]


LANES = 256
BLOCKS_A_STEP = 8


def gates(x, rw, iw, rb, ib, rate):
    tok, width = x.shape
    nb, bw = rw.shape[0], rw.shape[1]
    count = BLOCKS_A_STEP
    col = lambda rows: pl.BlockSpec((rows, count * bw), lambda b: (0, b))
    w = pl.BlockSpec((count, bw, bw), lambda b: (b, 0, 0))
    return pl.pallas_call(
        _gates_kernel,
        grid=(nb // count,),
        in_specs=[col(tok), w, w, col(1), col(1), col(1)],
        out_specs=[col(tok), col(tok), col(8), col(8), col(2)],
        out_shape=[
            jax.ShapeDtypeStruct((tok, width), F32),
            jax.ShapeDtypeStruct((tok, width), F32),
            jax.ShapeDtypeStruct((8, width), F32),
            jax.ShapeDtypeStruct((8, width), F32),
            jax.ShapeDtypeStruct((2, width), F32),
        ],
        scratch_shapes=[pltpu.VMEM((tok, tok), BF16), pltpu.VMEM((tok, count * bw), F32), pltpu.VMEM((tok, count * bw), F32)],
        compiler_params=pltpu.CompilerParams(dimension_semantics=("arbitrary",), vmem_limit_bytes=60 * 2**20),
        cost_estimate=pl.CostEstimate(flops=2 * 3 * tok * width * bw, bytes_accessed=2 * tok * width * 5, transcendentals=5 * tok * width),
        name="gates",
    )(x, rw, iw, rb.reshape(1, -1), ib.reshape(1, -1), rate.reshape(1, -1))


def _kv_kernel(state_ref, prod_ref, aex_ref, bex_ref, carry_ref, w_ref, hid_ref, kv_ref, acc_ref, h_ref, perm_ref):
    b = pl.program_id(0)

    @pl.when(b == 0)
    def _():
        perm_ref[...] = _perm_matrix(True)

    cc = bex_ref[...] + aex_ref[...] * carry_ref[...]
    for j in range(TOK // 8):
        row = slice(8 * j, 8 * j + 8)
        h_ref[row, :] = state_ref[row, :] + prod_ref[row, :] * cc
    hb = jnp.dot(perm_ref[...], h_ref[...].astype(BF16), preferred_element_type=F32).astype(BF16)
    hid_ref[...] = hb
    part = jnp.dot(hb, w_ref[...], preferred_element_type=F32)

    @pl.when(b == 0)
    def _():
        acc_ref[...] = part

    @pl.when(b > 0)
    def _():
        acc_ref[...] += part

    @pl.when(b == pl.num_programs(0) - 1)
    def _():
        hd = w_ref.shape[1] // 2
        k = acc_ref[:, :hd] * (LOG2E * hd ** -0.5)
        kv_ref[:hd, :] = k.T.astype(BF16)
        kv_ref[hd:, :] = acc_ref[:, hd:].astype(BF16)


def kv_project(state, prod, aex, bex, carry, w, bw=2048):
    tok, width = state.shape
    n = w.shape[1]
    col = lambda rows: pl.BlockSpec((rows, bw), lambda b: (0, b))
    return pl.pallas_call(
        _kv_kernel,
        grid=(width // bw,),
        in_specs=[col(tok), col(tok), col(8), col(8), col(1), pl.BlockSpec((bw, n), lambda b: (b, 0))],
        out_specs=[col(tok), pl.BlockSpec((n, tok), lambda b: (0, 0))],
        out_shape=[jax.ShapeDtypeStruct((tok, width), BF16), jax.ShapeDtypeStruct((n, tok), BF16)],
        scratch_shapes=[pltpu.VMEM((tok, n), F32), pltpu.VMEM((tok, bw), F32), pltpu.VMEM((tok, tok), BF16)],
        compiler_params=pltpu.CompilerParams(dimension_semantics=("arbitrary",), vmem_limit_bytes=60 * 2**20),
        cost_estimate=pl.CostEstimate(flops=2 * tok * width * n, bytes_accessed=10 * tok * width, transcendentals=0),
        name="kv_project",
    )(state, prod, aex, bex, carry, w)


class _Part:
    def __init__(self, count, edges, merge):
        self.count, self.edges, self.merge = count, edges, merge

    def scores(self, q, d, kv, bias_ref, s_ref):
        hd = kv[0].shape[0] // 2
        s = jnp.dot(q, kv[d][:hd, :], preferred_element_type=F32)
        s_ref[:, d * TOK:(d + 1) * TOK] = s if self.edges and d == 0 else s + bias_ref[d]

    def weights(self, r, s_ref, p_ref, r_ref, w_ref, tri_ref, lse_ref):
        cols = self.count * TOK
        at = slice(r, r + ROWS)
        row = slice(r % TOK, r % TOK + ROWS)
        lane = slice(r // TOK * 128, r // TOK * 128 + 128)
        last = cols - TOK
        merged = []
        if self.edges:
            keep = [tri_ref[row, c:c + 128] > 0.5 for c in range(0, TOK, 128)]
            merged = [
                jnp.where(keep[i], s_ref[at, 128 * i:128 * i + 128], s_ref[at, last + 128 * i:last + 128 * i + 128])
                for i in range(2)
            ]
        plain = range(TOK, last, 128) if self.edges else range(0, cols, 128)
        m = lse_ref[row, lane] if self.merge else None
        for v in merged:
            m = v if m is None else jnp.maximum(m, v)
        for c in plain:
            v = s_ref[at, c:c + 128]
            m = v if m is None else jnp.maximum(m, v)
        m = jnp.max(m, axis=1, keepdims=True)
        l = None
        for i, v in enumerate(merged):
            p = jnp.exp2(v - m)
            l = p if l is None else l + p
            p_ref[at, 128 * i:128 * i + 128] = jnp.where(keep[i], p, 0.0).astype(BF16)
            p_ref[at, last + 128 * i:last + 128 * i + 128] = jnp.where(keep[i], 0.0, p).astype(BF16)
        for c in plain:
            p = jnp.exp2(s_ref[at, c:c + 128] - m)
            l = p if l is None else l + p
            p_ref[at, c:c + 128] = p.astype(BF16)
        l = jnp.broadcast_to(jnp.sum(l, axis=1, keepdims=True), (ROWS, 128))
        if self.merge:
            before = jnp.exp2(lse_ref[row, lane] - m)
            l = l + before
            w_ref[at, :] = before / l
        else:
            lse_ref[row, lane] = m + jnp.log2(l)
        r_ref[at, :] = 1.0 / l

    def values(self, d, p_ref, kv):
        hd = kv[0].shape[0] // 2
        return jnp.dot(p_ref[:, d * TOK:(d + 1) * TOK], kv[d][hd:, :], preferred_element_type=F32)

    def kernel(self, bias_ref, q_ref, *refs):
        kv, refs = refs[:self.count], refs[self.count:]
        if self.merge:
            (lse_ref, before_ref, o_ref), refs = refs[:3], refs[3:]
        else:
            (o_ref, lse_ref), refs = refs[:2], refs[2:]
        s0, s1, p0, p1, r0, r1, w0, w1, tri_ref = refs
        s, p, inv, w = (s0, s1), (p0, p1), (r0, r1), (w0, w1)
        t = pl.program_id(0)
        last = pl.num_programs(0) - 3
        even = lax.rem(t, 2) == 0
        hd = kv[0].shape[0] // 2

        @pl.when(t == 0)
        def _():
            row = lax.broadcasted_iota(jnp.int32, (TOK, TOK), 0)
            col = lax.broadcasted_iota(jnp.int32, (TOK, TOK), 1)
            tri_ref[...] = (col <= row).astype(F32)

        def step(a, score, weigh, value):
            b = 1 - a
            total = UNIT * TOK // ROWS
            done, acc = 0, None
            if score:
                q = jnp.concatenate([q_ref[:, i * hd:(i + 1) * hd] for i in range(UNIT)], axis=0)
            for d in range(self.count):
                if score:
                    self.scores(q, d, kv, bias_ref, s[a])
                if value:
                    part = self.values(d, p[a], kv)
                    acc = part if acc is None else acc + part
                while weigh and done * self.count < (d + 1) * total:
                    self.weights(done * ROWS, s[b], p[b], inv[b], w[b], tri_ref, lse_ref)
                    done += 1
            if value:
                wide = lambda v: jnp.concatenate([v] * (hd // 128), axis=1)
                o = acc * wide(inv[a][...])
                for i in range(UNIT):
                    col, row = slice(i * hd, (i + 1) * hd), slice(i * TOK, (i + 1) * TOK)
                    part = o[row, :]
                    if self.merge:
                        part = part + before_ref[:, col] * wide(w[a][row, :])
                    o_ref[:, col] = part.astype(o_ref.dtype)

        pl.when(t == 0)(lambda: step(0, True, False, False))
        pl.when(t == 1)(lambda: step(1, True, True, False))
        pl.when((t >= 2) & (t <= last) & even)(lambda: step(0, True, True, True))
        pl.when((t >= 2) & (t <= last) & ~even)(lambda: step(1, True, True, True))
        pl.when(t == last + 1)(lambda: step(0, False, True, True))
        pl.when(t == last + 2)(lambda: step(1, False, False, True))

    def __call__(self, hidden, kv, bias, earlier=()):
        tok, width = hidden.shape
        hd = kv[0].shape[0] // 2
        heads = width // hd
        units = heads // UNIT
        unit = UNIT * tok
        block = lambda cols, lag: pl.BlockSpec((tok, UNIT * cols), lambda t, *_: (0, jnp.clip(t - lag, 0, units - 1)))
        result = jax.ShapeDtypeStruct((tok, width), BF16)
        out_specs, out_shape = block(hd, 2), result
        if not self.merge:
            out_specs = [block(hd, 2), block(128, 1)]
            out_shape = [jax.ShapeDtypeStruct((tok, width), F32), jax.ShapeDtypeStruct((tok, heads * 128), F32)]
        return pl.pallas_call(
            self.kernel,
            grid_spec=pltpu.PrefetchScalarGridSpec(
                num_scalar_prefetch=1,
                grid=(units + 2,),
                in_specs=[
                    block(hd, 0),
                    *[pl.BlockSpec((2 * hd, tok), lambda t, *_: (0, 0)) for _ in kv],
                    *([block(128, 1), block(hd, 2)] if self.merge else []),
                ],
                out_specs=out_specs,
                scratch_shapes=[
                    pltpu.VMEM((unit, self.count * tok), F32),
                    pltpu.VMEM((unit, self.count * tok), F32),
                    pltpu.VMEM((unit, self.count * tok), BF16),
                    pltpu.VMEM((unit, self.count * tok), BF16),
                    *[pltpu.VMEM((unit, 128), F32)] * 4,
                    pltpu.VMEM((tok, tok), F32),
                ],
            ),
            out_shape=out_shape,
            compiler_params=pltpu.CompilerParams(
                dimension_semantics=("arbitrary",),
                vmem_limit_bytes=ATTN_MIB * 2**20,
            ),
            cost_estimate=pl.CostEstimate(flops=4 * tok * width * self.count * tok, bytes_accessed=8 * tok * width, transcendentals=self.count * tok * tok * heads),
            name="attention_last" if self.merge else "attention_first",
        )(bias, hidden, *kv, *earlier)


ROWS = 32
UNIT = 2
ATTN_MIB = 32
HOIST = 2000


def attention(hidden, kv, bias):
    first, rest = [3, 4, 5, 6], [0, 1, 2, 7, 8]
    values, lse = _Part(4, False, False)(hidden, [kv[i] for i in first], jnp.stack([bias[i] for i in first]))
    return _Part(5, True, True)(hidden, [kv[i] for i in rest], jnp.stack([bias[i] for i in rest]), (lse, values))


def _after(earlier, later):
    return (earlier[0] * later[0], later[0] * earlier[1] + later[1])


def _kept(keep, pair):
    return (jnp.where(keep, pair[0], 1.0), jnp.where(keep, pair[1], 0.0))


def _shift(value, axis, distance):
    size = lax.axis_size(axis)
    return lax.ppermute(value, axis, [(i, (i + distance) % size) for i in range(size)])


def _entering(total):
    pair = lambda v: (v[0:1], v[1:2])
    packed = lambda p: jnp.concatenate(p)
    y, z = lax.axis_index("y"), lax.axis_index("z")
    ny, nz = lax.axis_size("y"), lax.axis_size("z")
    none = (jnp.ones_like(total[0:1]), jnp.zeros_like(total[0:1]))
    near = {k: pair(_shift(total, "y", k)) for k in range(ny - 1, 0, -1)}
    row = none
    for k in range(ny - 1, 0, -1):
        row = _after(row, _kept(y >= k, near[k]))
    whole = _after(row, pair(total))
    for k in range(ny - 1, 0, -1):
        whole = _after(whole, _kept(y < k, near[k]))
    if nz == 8:
        below = pair(_shift(packed(whole), "z", 1))
        above = pair(_shift(packed(whole), "z", -1))
        lower, upper = (z - 1) % nz, (z + 1) % nz

        def sent(target, rows):
            found = none
            for place, value in rows:
                found = _after(found, _kept(place < target, value))
            return packed(found)

        up = sent((z + 3) % nz, [(lower, below), (z, whole), (upper, above)])
        down = sent((z - 3) % nz, [(lower, below), (z, whole)])
        from_below = pair(_shift(up, "z", 3))
        from_above = pair(_shift(down, "z", -3))
        before = _kept(upper < z, above)
        for value in (from_above, from_below, _kept(lower < z, below)):
            before = _after(before, value)
    else:
        before, step = none, 1
        while step < nz:
            sent = packed(_after(before, whole))
            before = _after(_kept(z >= step, pair(_shift(sent, "z", step))), before)
            step *= 2
    return row[0] * before[1] + row[1]


def _window(kv):
    y = lax.axis_index("y")
    ny = lax.axis_size("y")
    one = _shift(kv, "z", 1)
    early = [(_shift(one, "y", k), jnp.where(y >= k, ny + k, k)) for k in (1, 3, 2)]
    two = _shift(one, "z", 1)
    late = [(_shift(jnp.where(y + k < ny, kv, two), "y", k), jnp.where(y >= k, k, ny + k)) for k in (1, 3, 2)]
    found = [*late[:2], (one, jnp.full((), ny, jnp.int32)), *early, late[2], (two, jnp.full((), 2 * ny, jnp.int32))]
    return [b for b, _ in found], [k for _, k in found]


def _on_device(inputs, recur_weight, input_weight, recur_bias, input_bias, decay_rate, kv_weight):
    state, prod, aex, bex, total = gates(inputs, recur_weight, input_weight, recur_bias, input_bias, decay_rate)
    carry = _entering(total)
    hidden, kv = kv_project(state, prod, aex, bex, carry, kv_weight)
    blocks, back = _window(kv)
    place = lax.axis_index("z") * lax.axis_size("y") + lax.axis_index("y")
    bias = [jnp.where(place >= k, 0.0, -1e30).astype(F32) for k in (jnp.zeros((), jnp.int32), *back)]
    return attention(hidden, [kv, *blocks], bias)


def solution(mesh):
    ny = 4
    nb, ns = mesh.shape["batch"], mesh.shape["seq"]
    names = mesh.axis_names
    order = {"seq": ("z", "y"), "batch": ("batch",)}
    sizes = {"seq": (ns // ny, ny), "batch": (nb,)}
    fine = jax.sharding.Mesh(
        mesh.devices.reshape([n for a in names for n in sizes[a]]),
        [a for n in names for a in order[n]],
    )
    rows = jax.sharding.PartitionSpec(("batch", "z", "y"), None)
    rep = jax.sharding.PartitionSpec()
    return jax.shard_map(
        _on_device, mesh=fine, in_specs=(rows, rep, rep, rep, rep, rep, rep), out_specs=rows, check_vma=False
    )
```
